32 devices in a mesh: row: 4 (over y, core), col: 8 (over z, x).
Axes of the slice: x: 2, y: 2, z: 4, core: 2. Of those that a mesh axis runs over, the one named last changes fastest.
Arguments:
- matrix: float32 [16384, 16384], P('row', 'col'), may hold values from -500 to 500
Outputs:
- reduced: float32 [16384, 16384], P('row', 'col')
The draws below stay inside these ranges and needn't reach their ends.
All inputs are finite; a program needn't handle non-finite values.
Results may differ from the reference program's by a relative error of at most 0.0003.
Values sent between devices are 32-bit elements; how exact they have to be, the bound alone decides.
A program may use at most 192 MiB of HBM per device.

```python
import math
import jax
import jax.numpy as jnp
from jax import lax

N = 16384
REFL = 4
PANELS = 2


def draw_matrix(key, part):
    scale_key = jax.random.fold_in(key, 11)
    noise_key = jax.random.fold_in(key, 12)
    diagonal_key = jax.random.fold_in(key, 14)
    position_ramp = jnp.arange(N, dtype=jnp.float32) / N
    spread = jnp.exp(jax.random.uniform(scale_key, (N,), jnp.float32, math.log(0.33), math.log(3.3)))
    scales = spread * jnp.exp(0.5 * math.log(3.0) * position_ramp)
    entries = jax.random.truncated_normal(noise_key, -6.0, 6.0, (N, N), jnp.float32)
    symmetric = (entries + entries.T) * 0.7071
    stiffness = jax.random.uniform(diagonal_key, (N,), jnp.float32, 2.0, 6.0)
    return scales[:, None] * symmetric * scales[None, :] + jnp.diag(stiffness * scales * scales)


def setup_inputs(seed: int = 0) -> dict:
    arg_keys = jax.random.split(jax.random.key(seed), 2)
    matrix = draw_matrix(jax.random.fold_in(arg_keys[1], 71), 0)
    return dict(matrix=matrix)


highest = lax.Precision.HIGHEST

def product(left, right):
    return jnp.dot(left, right, precision=highest, preferred_element_type=jnp.float32)

def reference(matrix):
    total = matrix.shape[0]
    positions = jnp.arange(total, dtype=jnp.int32)
    current = matrix
    for panel_index in range(PANELS):
        reflectors = jnp.zeros((total, REFL), jnp.float32)
        updates = jnp.zeros((total, REFL), jnp.float32)
        for inner_index in range(REFL):
            target = panel_index * REFL + inner_index
            column = current[:, target] - product(reflectors, updates[target]) - product(updates, reflectors[target])
            beneath = jnp.where(positions > target, column, 0.0)
            length = jnp.sqrt(jnp.sum(beneath * beneath))
            leading = column[target + 1]
            signed = jnp.where(leading >= 0.0, length, -length)
            vector = beneath + jnp.where(positions == target + 1, signed, 0.0)
            factor = 1.0 / (length * (length + jnp.abs(leading)))
            against_updates = product(vector, updates)
            against_reflectors = product(vector, reflectors)
            mapped = factor * (product(current, vector) - product(reflectors, against_updates) - product(updates, against_reflectors))
            update = mapped - 0.5 * factor * jnp.sum(mapped * vector) * vector
            reflectors = reflectors.at[:, inner_index].set(vector)
            updates = updates.at[:, inner_index].set(update)
        current = current - product(reflectors, updates.T) - product(updates, reflectors.T)
    return current
```

```python
import functools

import jax
import jax.numpy as jnp
from jax import lax
from jax.experimental import pallas as pl
from jax.experimental.pallas import tpu as pltpu
from jax.sharding import PartitionSpec as P

REFL = 4
PANELS = 2
STEPS = REFL * PANELS
LANES = 128
MESH = pl.DeviceIdType.MESH


def total_of(value):
    folded = jnp.sum(value, axis=0)
    folded = jnp.sum(folded, axis=0, keepdims=True)
    return jnp.sum(folded, axis=1, keepdims=True)


def kernel(
    nrow, ncol, a_hbm, v_ref, w_ref,
    a_vm, lead, rows, part, prod,
    load_sem, lead_sem,
    lead_send, lead_recv, rows_send, rows_recv,
    part_send, part_recv, prod_send, prod_recv,
):
    rows_local, cols_local = a_vm.shape
    kb = cols_local // LANES
    chunks = load_sem.shape[0]
    chunk = rows_local // chunks
    r = lax.axis_index("row")
    k = lax.axis_index("col")

    lead_load = pltpu.make_async_copy(a_hbm.at[pl.ds(0, STEPS), :], lead, lead_sem)
    lead_load.start()
    loads = []
    for n in range(chunks):
        span = pl.ds(n * chunk, chunk)
        load = pltpu.make_async_copy(a_hbm.at[span, :], a_vm.at[span, :], load_sem.at[n])
        load.start()
        loads.append(load)

    barrier = pltpu.get_barrier_semaphore()
    for d in range(1, nrow):
        pl.semaphore_signal(barrier, inc=1, device_id=(lax.rem(r + d, nrow), k), device_id_type=MESH)
    for d in range(1, ncol):
        pl.semaphore_signal(barrier, inc=1, device_id=(r, lax.rem(k + d, ncol)), device_id_type=MESH)

    v_ref[...] = jnp.zeros_like(v_ref)
    w_ref[...] = jnp.zeros_like(w_ref)
    lead_load.wait()

    @pl.when(r == 0)
    def _():
        for t in range(kb):
            rows[k, :, t, :] = lead[:, t * LANES:(t + 1) * LANES]

    pl.semaphore_wait(barrier, nrow + ncol - 2)

    def lead_copy(peer, n):
        return pltpu.make_async_remote_copy(
            src_ref=rows.at[k], dst_ref=rows.at[k],
            send_sem=lead_send.at[n], recv_sem=lead_recv,
            device_id=(peer, k), device_id_type=MESH,
        )

    @pl.when(r == 0)
    def _():
        for n in range(1, nrow):
            lead_copy(n, n).start()
        for n in range(1, nrow):
            lead_copy(n, n).wait_send()

    @pl.when(r != 0)
    def _():
        lead_copy(0, 0).wait_recv()

    def rows_copy(slot, peer, n):
        return pltpu.make_async_remote_copy(
            src_ref=rows.at[slot], dst_ref=rows.at[slot],
            send_sem=rows_send.at[n], recv_sem=rows_recv.at[slot],
            device_id=(r, peer), device_id_type=MESH,
        )

    for d in range(1, ncol):
        rows_copy(k, lax.rem(k + d, ncol), d).start()
    for d in range(1, ncol):
        rows_copy(k, lax.rem(k + d, ncol), d).wait_send()
        peer = lax.rem(k + ncol - d, ncol)
        rows_copy(peer, peer, d).wait_recv()
    for load in loads:
        load.wait()

    shape = (ncol, kb, LANES)
    positions = (
        lax.broadcasted_iota(jnp.int32, shape, 0) * cols_local
        + lax.broadcasted_iota(jnp.int32, shape, 1) * LANES
        + lax.broadcasted_iota(jnp.int32, shape, 2)
    )
    lane = lax.broadcasted_iota(jnp.int32, (1, LANES), 1)
    groups = rows_local // LANES

    def step(c, carry):
        column = rows[:, c]
        here = lane == c
        for i in range(STEPS):
            wc = jnp.sum(jnp.where(here, w_ref[i, 0, 0:1, :], 0.0), axis=1, keepdims=True)
            vc = jnp.sum(jnp.where(here, v_ref[i, 0, 0:1, :], 0.0), axis=1, keepdims=True)
            column = column - v_ref[i] * wc - w_ref[i] * vc
        beneath = jnp.where(positions > c, column, 0.0)
        leading = total_of(jnp.where(positions == c + 1, column, 0.0))
        length = jnp.sqrt(total_of(beneath * beneath))
        signed = jnp.where(leading >= 0.0, length, -length)
        vector = beneath + jnp.where(positions == c + 1, signed, 0.0)
        factor = 1.0 / (length * (length + jnp.abs(leading)))
        v_ref[c] = vector

        def group(j, sums):
            g = r * groups + j
            piece = v_ref[c, g // kb, pl.ds(g % kb, 1), :]
            spread = jnp.broadcast_to(piece, (LANES, LANES)).T
            base = pl.multiple_of(j * LANES, LANES)
            sums = list(sums)
            for b in range(LANES // 8):
                scale = spread[b * 8:(b + 1) * 8, :]
                for t in range(kb):
                    sums[t] = sums[t] + scale * a_vm[pl.ds(base + b * 8, 8), t * LANES:(t + 1) * LANES]
            return tuple(sums)

        sums = lax.fori_loop(
            0, groups, group, tuple(jnp.zeros((8, LANES), jnp.float32) for _ in range(kb))
        )
        for t in range(kb):
            part[c, r, t:t + 1, :] = jnp.sum(sums[t], axis=0, keepdims=True)

        def part_copy(slot, peer, n):
            return pltpu.make_async_remote_copy(
                src_ref=part.at[c, slot], dst_ref=part.at[c, slot],
                send_sem=part_send.at[n], recv_sem=part_recv.at[c, slot],
                device_id=(peer, k), device_id_type=MESH,
            )

        for d in range(1, nrow):
            part_copy(r, lax.rem(r + d, nrow), d).start()

        fixes = jnp.zeros(shape, jnp.float32)
        w_ref[c] = fixes
        for i in range(STEPS):
            old_v = v_ref[i]
            old_w = w_ref[i]
            fixes = fixes + old_v * total_of(old_w * vector) + old_w * total_of(old_v * vector)

        for d in range(1, nrow):
            peer = lax.rem(r + nrow - d, nrow)
            part_copy(peer, peer, d).wait_recv()
        summed = part[c, 0]
        for n in range(1, nrow):
            summed = summed + part[c, n]
        prod[c, k] = summed

        def prod_copy(slot, peer, n):
            return pltpu.make_async_remote_copy(
                src_ref=prod.at[c, slot], dst_ref=prod.at[c, slot],
                send_sem=prod_send.at[n], recv_sem=prod_recv.at[c, slot],
                device_id=(r, peer), device_id_type=MESH,
            )

        for d in range(1, ncol):
            prod_copy(k, lax.rem(k + d, ncol), d).start()
        for d in range(1, nrow):
            part_copy(r, lax.rem(r + d, nrow), d).wait_send()
        for d in range(1, ncol):
            peer = lax.rem(k + ncol - d, ncol)
            prod_copy(peer, peer, d).wait_recv()
        for d in range(1, ncol):
            prod_copy(k, lax.rem(k + d, ncol), d).wait_send()

        mapped = factor * (prod[c] - fixes)
        inner = total_of(mapped * vector)
        w_ref[c] = mapped - (0.5 * factor * inner) * vector
        return carry

    lax.fori_loop(0, STEPS, step, 0)


def reflectors_of(matrix, nrow, ncol):
    rows_local, cols_local = matrix.shape
    kb = cols_local // LANES
    vectors = jax.ShapeDtypeStruct((STEPS, ncol, kb, LANES), jnp.float32)
    dma = pltpu.SemaphoreType.DMA
    return pl.pallas_call(
        functools.partial(kernel, nrow, ncol),
        out_shape=(vectors, vectors),
        in_specs=[pl.BlockSpec(memory_space=pl.ANY)],
        out_specs=(pl.BlockSpec(memory_space=pltpu.VMEM),) * 2,
        scratch_shapes=[
            pltpu.VMEM((rows_local, cols_local), jnp.float32),
            pltpu.VMEM((STEPS, cols_local), jnp.float32),
            pltpu.VMEM((ncol, STEPS, kb, LANES), jnp.float32),
            pltpu.VMEM((STEPS, nrow, kb, LANES), jnp.float32),
            pltpu.VMEM((STEPS, ncol, kb, LANES), jnp.float32),
            dma((8,)), dma(()),
            dma((nrow,)), dma(()), dma((ncol,)), dma((ncol,)),
            dma((nrow,)), dma((STEPS, nrow)), dma((ncol,)), dma((STEPS, ncol)),
        ],
        compiler_params=pltpu.CompilerParams(
            collective_id=0, has_side_effects=True, vmem_limit_bytes=52 * 1024 * 1024
        ),
    )(matrix)


def thirds(value):
    first = lax.reduce_precision(value, 8, 7)
    rest = value - first
    second = lax.reduce_precision(rest, 8, 7)
    third = rest - second
    return [x.astype(jnp.bfloat16) for x in (first, second, third)]


def on_device(matrix):
    rows_local, cols_local = matrix.shape
    nrow, ncol = lax.axis_size("row"), lax.axis_size("col")
    reflectors, updates = reflectors_of(matrix, nrow, ncol)
    row_start = lax.axis_index("row") * rows_local
    flat_v = reflectors.reshape(STEPS, -1)
    flat_w = updates.reshape(STEPS, -1)
    left = jnp.concatenate([flat_v, flat_w], axis=0)
    left = lax.dynamic_slice_in_dim(left, row_start, rows_local, 1)
    col = lax.axis_index("col")
    right = jnp.concatenate(
        [lax.dynamic_index_in_dim(x, col, 1, keepdims=False).reshape(STEPS, cols_local)
         for x in (updates, reflectors)], axis=0)
    l1, l2, l3 = thirds(left)
    r1, r2, r3 = thirds(right)
    lefts = jnp.concatenate([l1, l1, l2, l2, l1, l3], axis=0)
    rights = jnp.concatenate([r1, r2, r1, r2, r3, r1], axis=0)
    change = lax.dot_general(
        lefts, rights, (((0,), (0,)), ((), ())), preferred_element_type=jnp.float32
    )
    return matrix - change


def solution(mesh):
    return jax.shard_map(
        on_device,
        mesh=mesh,
        in_specs=(P("row", "col"),),
        out_specs=P("row", "col"),
        check_vma=False,
    )
```
